64 devices in a mesh: dp: 4 (over x, y), tp: 16 (over z, core).
Axes of the slice: x: 2, y: 2, z: 8, core: 2. Of those that a mesh axis runs over, the one named last changes fastest.
The devices are a block of a 4x4x8 slice.
Arguments:
- x: bfloat16 [256, 2048], P('dp'), parts along dimension 0
- k_cache: bfloat16 [256, 2048, 16, 128], P('dp', None, 'tp'), parts along dimension 0
- v_cache: bfloat16 [256, 2048, 16, 128], P('dp', None, 'tp'), parts along dimension 0
- gain_a: bfloat16 [2048], replicated
- wq: bfloat16 [2048, 2048], P(None, 'tp')
- wo: bfloat16 [2048, 2048], P('tp')
- gain_m: bfloat16 [2048], replicated
- w_gate: bfloat16 [2048, 8192], P(None, 'tp')
- w_up: bfloat16 [2048, 8192], P(None, 'tp')
- w_down: bfloat16 [8192, 2048], P('tp')
Outputs:
- output: bfloat16 [256, 2048], P('dp'), parts along dimension 0
There are 4 independent parts. The reference program is written for one: setup_inputs(seed, part) draws one part's arguments, and reference() takes and returns one part's arrays. A program takes and returns all parts, laid end to end along the dimension named above; an argument that names none is the same for every part.
All inputs are finite; a program needn't handle non-finite values.
Results may differ from the reference program's by a relative error of at most 0.017.
Values are sent between devices in bfloat16 or wider.
A program may use at most 768 MiB of HBM per device.

```python
import jax
import jax.numpy as jnp
from jax import lax

BATCH = 64
CACHE = 2048
D = 2048
HEADS = 16
KV_HEADS = 16
HEAD = 128
FF = 8192
THETA = 10000


def setup_inputs(seed: int = 0, part: int = 0) -> dict:
    kx, kc, kw, kn, kq, ko, km, kg, ku, kd = jax.random.split(jax.random.key(seed), 10)
    kx, kc, kw = (jax.random.fold_in(k, part) for k in (kx, kc, kw))

    def weights(key, rows, columns):
        return jax.random.normal(key, (rows, columns), jnp.float32) * rows**-0.5

    drawn = {
        "x": jax.random.normal(kx, (BATCH, D), jnp.float32),
        "k_cache": 2 * jax.random.normal(kc, (BATCH, CACHE, KV_HEADS, HEAD), jnp.float32),
        "v_cache": 4 * jax.random.normal(kw, (BATCH, CACHE, KV_HEADS, HEAD), jnp.float32),
        "gain_a": 1 + 0.1 * jax.random.normal(kn, (D,), jnp.float32),
        "wq": 2 * weights(kq, D, HEADS * HEAD),
        "wo": weights(ko, HEADS * HEAD, D),
        "gain_m": 1 + 0.1 * jax.random.normal(km, (D,), jnp.float32),
        "w_gate": weights(kg, D, FF),
        "w_up": weights(ku, D, FF),
        "w_down": 2 * weights(kd, FF, D),
    }
    return {k: v.astype(jnp.bfloat16) for k, v in drawn.items()}


def normed(x, gain):
    wide = x.astype(jnp.float32)
    scale = lax.rsqrt(jnp.mean(wide * wide, -1, keepdims=True) + 1e-6)
    return (wide * scale * gain.astype(jnp.float32)).astype(jnp.bfloat16)


def turned(t, place, theta):
    half = t.shape[-1] // 2
    angle = place.astype(jnp.float32)[:, None] * theta ** (-jnp.arange(half, dtype=jnp.float32) / half)
    cos, sin = jnp.cos(angle)[:, None], jnp.sin(angle)[:, None]
    a, b = t[..., :half].astype(jnp.float32), t[..., half:].astype(jnp.float32)
    return jnp.concatenate([a * cos - b * sin, b * cos + a * sin], -1).astype(jnp.bfloat16)


def matmul(a, w):
    return jnp.dot(a, w, preferred_element_type=jnp.float32).astype(jnp.bfloat16)


def einsum(form, a, b):
    return jnp.einsum(form, a.astype(jnp.float32), b.astype(jnp.float32))


def seen_by(a, wq, k_cache, v_cache, head, theta):
    batch, cache, kv_heads = k_cache.shape[:3]
    place = jnp.full((batch,), cache - 1)
    q = turned(matmul(a, wq).reshape(batch, -1, head), place, theta).reshape(batch, kv_heads, -1, head)
    scores = einsum("bgsd,bugd->bgsu", q, k_cache) * head**-0.5
    weights = jax.nn.softmax(scores, -1).astype(jnp.bfloat16)
    return einsum("bgsu,bugd->bgsd", weights, v_cache).astype(jnp.bfloat16).reshape(batch, -1)


def hidden_of(b, w_gate, w_up):
    gate = jnp.dot(b, w_gate, preferred_element_type=jnp.float32)
    up = jnp.dot(b, w_up, preferred_element_type=jnp.float32)
    return (jax.nn.silu(gate) * up).astype(jnp.bfloat16)


def reference(x, k_cache, v_cache, gain_a, wq, wo, gain_m, w_gate, w_up, w_down):
    seen = seen_by(normed(x, gain_a), wq, k_cache, v_cache, HEAD, THETA)
    h = (x.astype(jnp.float32) + jnp.dot(seen, wo, preferred_element_type=jnp.float32)).astype(jnp.bfloat16)
    hidden = hidden_of(normed(h, gain_m), w_gate, w_up)
    return (h.astype(jnp.float32) + jnp.dot(hidden, w_down, preferred_element_type=jnp.float32)).astype(jnp.bfloat16)
```

```python
import functools

import jax
import jax.numpy as jnp
import numpy as np
from jax import lax
from jax.experimental import pallas as pl
from jax.experimental.pallas import tpu as pltpu
from jax.sharding import PartitionSpec as P

HEAD = 128
THETA = 10000
CHUNK = 16
SLOTS = 3
TILE = 256
EPS = 1e-6
MESH = pl.DeviceIdType.MESH
F32, BF16 = jnp.float32, jnp.bfloat16


def far_first(n):
    return sorted(range(1, n), key=lambda d: -min(d, n - d))


def kernel(n, x_hbm, k_hbm, v_hbm, ga_hbm, wq_hbm, wo_hbm, gm_hbm, wg_hbm, wu_hbm, wd_hbm, rot_hbm, out_ref,
           kbuf, vbuf, x_v, a_v, ga_v, gm_v, rot_v, wq_v, wo_v, wg_v, wu_v, wd_v, q_v, s_v, p_v, f_v, own_v, hown_v,
           t1, r1, hh, t2, r2, yy, ksem, vsem, wsem, send_sem, recv_sem):
    me = lax.axis_index("tp")
    rows, d_model = x_v.shape
    chunks = rows // CHUNK
    cache = kbuf.shape[2]
    pairs = CHUNK // 2
    width = d_model // n

    barrier = pltpu.get_barrier_semaphore()
    for d in range(1, n):
        pl.semaphore_signal(barrier, inc=1, device_id={"tp": lax.rem(me + d, n)}, device_id_type=MESH)

    small = [(x_hbm, x_v), (wq_hbm, wq_v), (ga_hbm, ga_v), (rot_hbm, rot_v), (wo_hbm, wo_v), (gm_hbm, gm_v),
             (wg_hbm, wg_v), (wu_hbm, wu_v), (wd_hbm, wd_v)]

    def load(i):
        return pltpu.make_async_copy(small[i][0], small[i][1], wsem.at[i])

    def kv(hbm, buf, sem, c, j):
        slot = lax.rem(c, SLOTS)
        return pltpu.make_async_copy(hbm.at[pl.ds(c * CHUNK + 2 * j, 2)], buf.at[slot, pl.ds(2 * j, 2)], sem.at[slot, j])

    def start_k(c):
        for j in range(pairs):
            kv(k_hbm, kbuf, ksem, c, j).start()

    def start_v(c):
        for j in range(pairs):
            kv(v_hbm, vbuf, vsem, c, j).start()

    for i in range(4):
        load(i).start()
    for c in range(min(SLOTS, chunks)):
        start_k(c)
        start_v(c)
        if c == 0:
            load(4).start()
            load(5).start()
        if c == 1:
            for i in range(6, 9):
                load(i).start()

    for i in range(4):
        load(i).wait()
    gain_a = ga_v[...].astype(F32)
    for c in range(chunks):
        wide = x_v[c * CHUNK:(c + 1) * CHUNK, :].astype(F32)
        scale = lax.rsqrt(jnp.mean(wide * wide, -1, keepdims=True) + EPS)
        a_v[c * CHUNK:(c + 1) * CHUNK, :] = (wide * scale * gain_a).astype(BF16)
    q = jnp.dot(a_v[...], wq_v[...], preferred_element_type=F32).astype(BF16).astype(F32)
    q_v[...] = (q * rot_v[0:1, :] + pltpu.roll(q, HEAD // 2, 1) * rot_v[1:2, :]).astype(BF16)

    row = lax.broadcasted_iota(jnp.int32, (CHUNK, HEAD), 0)

    def send_all(phase, c, source, target):
        for d in far_first(n):
            to = lax.rem(me + d, n)
            pltpu.make_async_remote_copy(
                src_ref=source(to, d), dst_ref=target(to, d), send_sem=send_sem.at[phase, c], recv_sem=recv_sem.at[phase, c],
                device_id={"tp": to}, device_id_type=MESH).start()

    def arrived(phase, c, ref):
        block = ref.at[c, pl.ds(0, n - 1)]
        pltpu.make_async_remote_copy(
            src_ref=block, dst_ref=block, send_sem=send_sem.at[phase, c], recv_sem=recv_sem.at[phase, c],
            device_id={"tp": me}, device_id_type=MESH).wait_recv()

    def sent(phase, c, ref):
        block = ref.at[c, pl.ds(0, n - 1)]
        pltpu.make_async_remote_copy(
            src_ref=block, dst_ref=block, send_sem=send_sem.at[phase, c], recv_sem=recv_sem.at[phase, c],
            device_id={"tp": me}, device_id_type=MESH).wait_send()

    def scatter(phase, c, term, t, r):
        for k in range(n):
            part = term[:, k * width:(k + 1) * width]
            f_v[k] = part
            t[c, k] = part.astype(BF16)
        own_v[phase // 2, c] = f_v[me]
        send_all(phase, c, lambda to, d: t.at[c, to], lambda to, d: r.at[c, d - 1])

    def gathered(phase, c, r):
        arrived(phase, c, r)
        total = own_v[phase // 2, c]
        for d in range(n - 1):
            total = total + r[c, d].astype(F32)
        return total

    def attention(c):
        slot = lax.rem(c, SLOTS)
        queries = q_v[pl.ds(pl.multiple_of(c * CHUNK, CHUNK), CHUNK), :].astype(F32)
        for j in range(pairs):
            kv(k_hbm, kbuf, ksem, c, j).wait()
            both = jnp.concatenate([jnp.where(row == 2 * j, queries, 0.0), jnp.where(row == 2 * j + 1, queries, 0.0)], -1).astype(BF16)
            for t in range(0, cache, TILE):
                keys = jnp.concatenate([kbuf[slot, 2 * j, t:t + TILE, :], kbuf[slot, 2 * j + 1, t:t + TILE, :]], -1)
                part = lax.dot_general(both, keys, (((1,), (1,)), ((), ())), preferred_element_type=F32)
                if j == 0:
                    s_v[:, t:t + TILE] = part
                else:
                    s_v[:, t:t + TILE] += part

        @pl.when(c + SLOTS < chunks)
        def _():
            start_k(c + SLOTS)

        scores = s_v[...] * HEAD**-0.5
        e = jnp.exp(scores - jnp.max(scores, -1, keepdims=True))
        p_v[...] = (e / jnp.sum(e, -1, keepdims=True)).astype(BF16)
        seen = jnp.zeros((CHUNK, HEAD), F32)
        for j in range(pairs):
            kv(v_hbm, vbuf, vsem, c, j).wait()
            values = jnp.concatenate([vbuf[slot, 2 * j], vbuf[slot, 2 * j + 1]], -1)
            both = jnp.dot(p_v[...], values, preferred_element_type=F32)
            seen = jnp.where(row == 2 * j, both[:, :HEAD], seen)
            seen = jnp.where(row == 2 * j + 1, both[:, HEAD:], seen)

        @pl.when(c + SLOTS < chunks)
        def _():
            start_v(c + SLOTS)

        @pl.when(c == 0)
        def _():
            load(4).wait()
            pl.semaphore_wait(barrier, n - 1)

        scatter(0, c, jnp.dot(seen.astype(BF16), wo_v[...], preferred_element_type=F32), t1, r1)

    def finish_h(c):
        mine = x_v[pl.ds(pl.multiple_of(c * CHUNK, CHUNK), CHUNK), pl.ds(pl.multiple_of(me * width, width), width)]
        h = (mine.astype(F32) + gathered(0, c, r1)).astype(BF16)
        hown_v[c] = h
        hh[c, me] = h
        send_all(1, c, lambda to, d: hh.at[c, me], lambda to, d: hh.at[c, me])

    def mlp(c):
        @pl.when(c == 0)
        def _():
            for i in range(5, 9):
                load(i).wait()

        arrived(1, c, hh)
        squares = jnp.zeros((CHUNK, width), F32)
        for k in range(n):
            wide = hh[c, k].astype(F32)
            squares = squares + wide * wide
        scale = lax.rsqrt(jnp.sum(squares, -1, keepdims=True) / d_model + EPS)
        b = jnp.concatenate(
            [(hh[c, k].astype(F32) * scale * gm_v[:, k * width:(k + 1) * width].astype(F32)).astype(BF16) for k in range(n)], -1)
        gate = jnp.dot(b, wg_v[...], preferred_element_type=F32)
        up = jnp.dot(b, wu_v[...], preferred_element_type=F32)
        hidden = (gate * jax.nn.sigmoid(gate) * up).astype(BF16)
        scatter(2, c, jnp.dot(hidden, wd_v[...], preferred_element_type=F32), t2, r2)

    def finish_y(c):
        yy[c, me] = (hown_v[c].astype(F32) + gathered(2, c, r2)).astype(BF16)
        send_all(3, c, lambda to, d: yy.at[c, me], lambda to, d: yy.at[c, me])

    def step(s, carry):
        for lag, stage in enumerate((attention, finish_h, mlp, finish_y)):
            @pl.when((s >= lag) & (s < chunks + lag))
            def _(stage=stage, lag=lag):
                stage(s - lag)

        return carry

    lax.fori_loop(0, chunks + 3, step, 0)

    for c in range(chunks):
        arrived(3, c, yy)
        for k in range(n):
            out_ref[c * CHUNK:(c + 1) * CHUNK, k * width:(k + 1) * width] = yy[c, k]
    for c in range(chunks):
        for phase, ref in enumerate((t1, hh, t2, yy)):
            sent(phase, c, ref)


def rotation(place):
    half = HEAD // 2
    angle = np.float64(place) * float(THETA) ** (-np.arange(half) / half)
    cos, sin = np.cos(angle), np.sin(angle)
    table = np.zeros((8, HEAD), np.float32)
    table[0], table[1] = np.concatenate([cos, cos]), np.concatenate([-sin, sin])
    return table


def solution(mesh):
    n = mesh.shape["tp"]

    def step(x, k_cache, v_cache, gain_a, wq, wo, gain_m, w_gate, w_up, w_down):
        rows, d_model = x.shape
        cache = k_cache.shape[1]
        chunks, hidden, width = rows // CHUNK, w_gate.shape[1], d_model // n
        anywhere = pl.BlockSpec(memory_space=pl.ANY)
        tiles = pltpu.VMEM((chunks, n, CHUNK, width), BF16)
        arrivals = pltpu.VMEM((chunks, n - 1, CHUNK, width), BF16)
        dma = pltpu.SemaphoreType.DMA
        return pl.pallas_call(
            functools.partial(kernel, n),
            out_shape=jax.ShapeDtypeStruct((rows, d_model), BF16),
            in_specs=[anywhere] * 11,
            out_specs=pl.BlockSpec(memory_space=pltpu.VMEM),
            scratch_shapes=[
                pltpu.VMEM((SLOTS, CHUNK, cache, HEAD), BF16),
                pltpu.VMEM((SLOTS, CHUNK, cache, HEAD), BF16),
                pltpu.VMEM((rows, d_model), BF16),
                pltpu.VMEM((rows, d_model), BF16),
                pltpu.VMEM((1, d_model), BF16),
                pltpu.VMEM((1, d_model), BF16),
                pltpu.VMEM((8, HEAD), F32),
                pltpu.VMEM(wq.shape, BF16),
                pltpu.VMEM(wo.shape, BF16),
                pltpu.VMEM((d_model, hidden), BF16),
                pltpu.VMEM((d_model, hidden), BF16),
                pltpu.VMEM((hidden, d_model), BF16),
                pltpu.VMEM((rows, HEAD), BF16),
                pltpu.VMEM((CHUNK, cache), F32),
                pltpu.VMEM((CHUNK, cache), BF16),
                pltpu.VMEM((n, CHUNK, width), F32),
                pltpu.VMEM((2, chunks, CHUNK, width), F32),
                pltpu.VMEM((chunks, CHUNK, width), BF16),
                tiles, arrivals, tiles, tiles, arrivals, tiles,
                dma((SLOTS, CHUNK // 2)), dma((SLOTS, CHUNK // 2)), dma((9,)), dma((4, chunks)), dma((4, chunks)),
            ],
            compiler_params=pltpu.CompilerParams(collective_id=0, has_side_effects=True, vmem_limit_bytes=67043328),
        )(x, k_cache.reshape(rows, cache, HEAD), v_cache.reshape(rows, cache, HEAD), gain_a.reshape(1, -1), wq, wo,
          gain_m.reshape(1, -1), w_gate, w_up, w_down, jnp.asarray(rotation(cache - 1)))

    states, cache, columns, rows_of = P("dp", None), P("dp", None, "tp", None), P(None, "tp"), P("tp", None)
    return jax.shard_map(
        step,
        mesh=mesh,
        in_specs=(states, cache, cache, P(None), columns, rows_of, P(None), columns, columns, rows_of),
        out_specs=states,
        check_vma=False,
    )
```

```python
import functools

import jax
import jax.numpy as jnp
import numpy as np
from jax import lax
from jax.experimental import pallas as pl
from jax.experimental.pallas import tpu as pltpu
from jax.sharding import PartitionSpec as P

HEAD = 128
THETA = 10000
CHUNK = 16
SLOTS = 2
AHEAD = 16
FIRST = 4
GROUP = 4
VMEM_LIMIT = 48 << 20
TILE = 256
EPS = 1e-6
MESH = pl.DeviceIdType.MESH
F32, BF16 = jnp.float32, jnp.bfloat16


def far_first(n):
    return sorted(range(1, n), key=lambda d: -min(d, n - d))


def kernel(n, x_hbm, k_hbm, v_hbm, ga_hbm, wq_hbm, wo_hbm, gm_hbm, wg_hbm, wu_hbm, wd_hbm, rot_hbm, out_ref,
           kbuf, vbuf, x_v, a_v, ga_v, gm_v, rot_v, wq_v, wo_v, wg_v, wu_v, wd_v, q_v, s_v, p_v, f_v, own_v, hown_v,
           t1, r1, hh, t2, r2, yy, ksem, vsem, wsem, send_sem, recv_sem):
    me = lax.axis_index("tp")
    rows, d_model = x_v.shape
    chunks = rows // CHUNK
    cache = kbuf.shape[2]
    pairs = CHUNK // 2
    width = d_model // n

    barrier = pltpu.get_barrier_semaphore()
    for d in range(1, n):
        pl.semaphore_signal(barrier, inc=1, device_id={"tp": lax.rem(me + d, n)}, device_id_type=MESH)

    small = [(x_hbm, x_v), (wq_hbm, wq_v), (ga_hbm, ga_v), (rot_hbm, rot_v), (wo_hbm, wo_v), (gm_hbm, gm_v),
             (wg_hbm, wg_v), (wu_hbm, wu_v), (wd_hbm, wd_v)]

    def load(i):
        return pltpu.make_async_copy(small[i][0], small[i][1], wsem.at[i])

    def kv(hbm, buf, sem, c, j):
        slot = lax.rem(c, SLOTS)
        return pltpu.make_async_copy(hbm.at[pl.ds(c * CHUNK + 2 * j, 2)], buf.at[slot, pl.ds(2 * j, 2)], sem.at[slot, j])

    def item(c, i):
        c, i = c + i // (2 * pairs), i % (2 * pairs)
        return kv(k_hbm, kbuf, ksem, c, i) if i < pairs else kv(v_hbm, vbuf, vsem, c, i - pairs)

    def refill(c, i):
        ramp = 2 * i + pairs + 1 <= i + AHEAD

        @pl.when(c == 0)
        def _():
            for m in (2 * i + pairs, 2 * i + pairs + 1) if ramp else (i + AHEAD,):
                item(0, m).start()

        @pl.when((c > 0) & (c + (i + AHEAD) // (2 * pairs) < chunks))
        def _():
            item(c, i + AHEAD).start()

    for i in range(4):
        load(i).start()
    for i in range(FIRST):
        item(0, i).start()

    with jax.named_scope("wait_x"):
        for i in (0, 2):
            load(i).wait()
    for c in range(chunks):
        wide = x_v[c * CHUNK:(c + 1) * CHUNK, :].astype(F32)
        scale = lax.rsqrt(jnp.mean(wide * wide, -1, keepdims=True) + EPS)
        for k in range(n):
            block = pl.ds(k * width, width)
            a_v[c * CHUNK:(c + 1) * CHUNK, block] = (wide[:, k * width:(k + 1) * width] * scale * ga_v[k:k + 1, :].astype(F32)).astype(BF16)
    with jax.named_scope("wait_wq"):
        for i in (1, 3):
            load(i).wait()
    load(4).start()
    for i in range(FIRST, pairs):
        item(0, i).start()
    q = jnp.dot(a_v[...], wq_v[...], preferred_element_type=F32).astype(BF16).astype(F32)
    q_v[...] = (q * rot_v[0:1, :] + pltpu.roll(q, HEAD // 2, 1) * rot_v[1:2, :]).astype(BF16)

    row = lax.broadcasted_iota(jnp.int32, (CHUNK, HEAD), 0)

    def send_all(phase, c, source, target):
        for d in far_first(n):
            to = lax.rem(me + d, n)
            pltpu.make_async_remote_copy(
                src_ref=source(to, d), dst_ref=target(to, d), send_sem=send_sem.at[phase, c], recv_sem=recv_sem.at[phase, c],
                device_id={"tp": to}, device_id_type=MESH).start()

    def arrived(phase, c, ref):
        block = ref.at[c, pl.ds(0, n - 1)]
        pltpu.make_async_remote_copy(
            src_ref=block, dst_ref=block, send_sem=send_sem.at[phase, c], recv_sem=recv_sem.at[phase, c],
            device_id={"tp": me}, device_id_type=MESH).wait_recv()

    def sent(phase, c, ref):
        block = ref.at[c, pl.ds(0, n - 1)]
        pltpu.make_async_remote_copy(
            src_ref=block, dst_ref=block, send_sem=send_sem.at[phase, c], recv_sem=recv_sem.at[phase, c],
            device_id={"tp": me}, device_id_type=MESH).wait_send()

    def split(phase, c, term, t):
        for k in range(n):
            part = term[:, k * width:(k + 1) * width]
            f_v[k] = part
            t[c, k] = part.astype(BF16)
        own_v[phase // 2, c] = f_v[me]

    def scatter(phase, c, t, r):
        send_all(phase, c, lambda to, d: t.at[c, to], lambda to, d: r.at[c, d - 1])

    def gathered(phase, c, r):
        with jax.named_scope("wait_terms"):
            arrived(phase, c, r)
        total = own_v[phase // 2, c]
        for d in range(n - 1):
            total = total + r[c, d].astype(F32)
        return total

    def attention(c):
        slot = lax.rem(c, SLOTS)
        queries = q_v[pl.ds(pl.multiple_of(c * CHUNK, CHUNK), CHUNK), :].astype(F32)
        for j in range(pairs):
            with jax.named_scope("wait_k"):
                kv(k_hbm, kbuf, ksem, c, j).wait()
            refill(c, j)
            with jax.named_scope("scores"):
                both = jnp.concatenate([jnp.where(row == 2 * j, queries, 0.0), jnp.where(row == 2 * j + 1, queries, 0.0)], -1).astype(BF16)
                for t in range(0, cache, TILE):
                    keys = jnp.concatenate([kbuf[slot, 2 * j, t:t + TILE, :], kbuf[slot, 2 * j + 1, t:t + TILE, :]], -1)
                    part = lax.dot_general(both, keys, (((1,), (1,)), ((), ())), preferred_element_type=F32)
                    if j == 0:
                        s_v[:, t:t + TILE] = part
                    else:
                        s_v[:, t:t + TILE] += part

        @pl.when(c == 0)
        def _():
            load(4).wait()
            with jax.named_scope("barrier"):
                pl.semaphore_wait(barrier, n - 1)

        @pl.when(c >= 2)
        def _():
            finish_h(c - 2)

        with jax.named_scope("softmax"):
            scores = s_v[...] * HEAD**-0.5
            e = jnp.exp(scores - jnp.max(scores, -1, keepdims=True))
            p_v[...] = (e / jnp.sum(e, -1, keepdims=True)).astype(BF16)
        seen = jnp.zeros((CHUNK, HEAD), F32)
        for j in range(0, pairs, GROUP):
            with jax.named_scope("wait_v"):
                for i in range(j, j + GROUP):
                    kv(v_hbm, vbuf, vsem, c, i).wait()
            for i in range(j, j + GROUP):
                refill(c, pairs + i)
            if j + GROUP == pairs:
                @pl.when(c == chunks - 1)
                def _():
                    for i in range(5, 9):
                        load(i).start()

            with jax.named_scope("values"):
                values = jnp.concatenate([vbuf[slot, 2 * j + i] for i in range(2 * GROUP)], -1)
                each = jnp.dot(p_v[...], values, preferred_element_type=F32)
                for i in range(2 * GROUP):
                    seen = jnp.where(row == 2 * j + i, each[:, i * HEAD:(i + 1) * HEAD], seen)

        with jax.named_scope("wo"):
            split(0, c, jnp.dot(seen.astype(BF16), wo_v[...], preferred_element_type=F32), t1)
            scatter(0, c, t1, r1)

    def finish_h(c):
        mine = x_v[pl.ds(pl.multiple_of(c * CHUNK, CHUNK), CHUNK), pl.ds(pl.multiple_of(me * width, width), width)]
        h = (mine.astype(F32) + gathered(0, c, r1)).astype(BF16)
        hown_v[c] = h
        hh[c, me] = h
        send_all(1, c, lambda to, d: hh.at[c, me], lambda to, d: hh.at[c, me])

    def normed(c):
        with jax.named_scope("wait_h"):
            arrived(1, c, hh)
        squares = jnp.zeros((CHUNK, width), F32)
        for k in range(n):
            wide = hh[c, k].astype(F32)
            squares = squares + wide * wide
        scale = lax.rsqrt(jnp.sum(squares, -1, keepdims=True) / d_model + EPS)
        return jnp.concatenate([(hh[c, k].astype(F32) * scale * gm_v[k:k + 1, :].astype(F32)).astype(BF16) for k in range(n)], -1)

    def mlp(*which):
        b = jnp.concatenate([normed(c) for c in which], 0)
        with jax.named_scope("mlp"):
            gate = jnp.dot(b, wg_v[...], preferred_element_type=F32)
            up = jnp.dot(b, wu_v[...], preferred_element_type=F32)
            hidden = (gate * jax.nn.sigmoid(gate) * up).astype(BF16)
            term = jnp.dot(hidden, wd_v[...], preferred_element_type=F32)
            for i, c in enumerate(which):
                split(2, c, term[i * CHUNK:(i + 1) * CHUNK], t2)

    def finish_y(c):
        yy[c, me] = (hown_v[c].astype(F32) + gathered(2, c, r2)).astype(BF16)
        send_all(3, c, lambda to, d: yy.at[c, me], lambda to, d: yy.at[c, me])

    def step(c, carry):
        attention(c)
        return carry

    lax.fori_loop(0, chunks, step, 0)

    *early, late, last = range(chunks)
    finish_h(late)
    with jax.named_scope("wait_w"):
        for i in range(5, 9):
            load(i).wait()
    mlp(*early)
    finish_h(last)
    for c in early:
        scatter(2, c, t2, r2)
    mlp(late)
    scatter(2, late, t2, r2)
    mlp(last)
    scatter(2, last, t2, r2)
    for c in (*early, late, last):
        finish_y(c)

    for c in range(chunks):
        if c == last:
            for i in range(chunks):
                for phase, ref in enumerate((t1, hh, t2)):
                    sent(phase, i, ref)
                if i != last:
                    sent(3, i, yy)
        with jax.named_scope("wait_y"):
            arrived(3, c, yy)
        for k in range(n):
            out_ref[c * CHUNK:(c + 1) * CHUNK, k * width:(k + 1) * width] = yy[c, k]
    sent(3, last, yy)


def rotation(place):
    half = HEAD // 2
    angle = np.float64(place) * float(THETA) ** (-np.arange(half) / half)
    cos, sin = np.cos(angle), np.sin(angle)
    table = np.zeros((8, HEAD), np.float32)
    table[0], table[1] = np.concatenate([cos, cos]), np.concatenate([-sin, sin])
    return table


def solution(mesh):
    n = mesh.shape["tp"]

    def step(x, k_cache, v_cache, gain_a, wq, wo, gain_m, w_gate, w_up, w_down):
        rows, d_model = x.shape
        cache = k_cache.shape[1]
        chunks, hidden, width = rows // CHUNK, w_gate.shape[1], d_model // n
        anywhere = pl.BlockSpec(memory_space=pltpu.HBM)
        tiles = pltpu.VMEM((chunks, n, CHUNK, width), BF16)
        arrivals = pltpu.VMEM((chunks, n - 1, CHUNK, width), BF16)
        dma = pltpu.SemaphoreType.DMA
        return pl.pallas_call(
            functools.partial(kernel, n),
            out_shape=jax.ShapeDtypeStruct((rows, d_model), BF16),
            in_specs=[anywhere] * 11,
            out_specs=pl.BlockSpec(memory_space=pltpu.VMEM),
            scratch_shapes=[
                pltpu.VMEM((SLOTS, CHUNK, cache, HEAD), BF16),
                pltpu.VMEM((SLOTS, CHUNK, cache, HEAD), BF16),
                pltpu.VMEM((rows, d_model), BF16),
                pltpu.VMEM((rows, d_model), BF16),
                pltpu.VMEM((n, width), BF16),
                pltpu.VMEM((n, width), BF16),
                pltpu.VMEM((8, HEAD), F32),
                pltpu.VMEM(wq.shape, BF16),
                pltpu.VMEM(wo.shape, BF16),
                pltpu.VMEM((d_model, hidden), BF16),
                pltpu.VMEM((d_model, hidden), BF16),
                pltpu.VMEM((hidden, d_model), BF16),
                pltpu.VMEM((rows, HEAD), BF16),
                pltpu.VMEM((CHUNK, cache), F32),
                pltpu.VMEM((CHUNK, cache), BF16),
                pltpu.VMEM((n, CHUNK, width), F32),
                pltpu.VMEM((2, chunks, CHUNK, width), F32),
                pltpu.VMEM((chunks, CHUNK, width), BF16),
                tiles, arrivals, tiles, tiles, arrivals, tiles,
                dma((SLOTS, CHUNK // 2)), dma((SLOTS, CHUNK // 2)), dma((9,)), dma((4, chunks)), dma((4, chunks)),
            ],
            compiler_params=pltpu.CompilerParams(collective_id=0, has_side_effects=True, vmem_limit_bytes=VMEM_LIMIT),
        )(*(pltpu.with_memory_space_constraint(a, pltpu.HBM) for a in (
            x, k_cache.reshape(rows, cache, HEAD), v_cache.reshape(rows, cache, HEAD), gain_a.reshape(n, width), wq, wo,
            gain_m.reshape(n, width), w_gate, w_up, w_down, jnp.asarray(rotation(cache - 1)))))

    states, cache, columns, rows_of = P("dp", None), P("dp", None, "tp", None), P(None, "tp"), P("tp", None)
    return jax.shard_map(
        step,
        mesh=mesh,
        in_specs=(states, cache, cache, P(None), columns, rows_of, P(None), columns, columns, rows_of),
        out_specs=states,
        check_vma=False,
    )
```

```python
import functools

import jax
import jax.numpy as jnp
import numpy as np
from jax import lax
from jax.experimental import pallas as pl
from jax.experimental.pallas import tpu as pltpu
from jax.sharding import PartitionSpec as P

HEAD = 128
THETA = 10000
CHUNK = 16
SLOTS = 2
AHEAD = 16
FIRST = 4
GROUP = 4
VMEM_LIMIT = 48 << 20
TILE = 256
EPS = 1e-6
MESH = pl.DeviceIdType.MESH
F32, BF16 = jnp.float32, jnp.bfloat16


def paired(early, late, last):
    return [(1, late), (2, late), (3, late), *((phase, c) for phase in (2, 3) for c in early)]


def far_first(n):
    return sorted(range(1, n), key=lambda d: -min(d, n - d))


def kernel(n, x_hbm, k_hbm, v_hbm, ga_hbm, wq_hbm, wo_hbm, gm_hbm, wg_hbm, wu_hbm, wd_hbm, rot_hbm, out_ref,
           kbuf, vbuf, x_v, a_v, ga_v, gm_v, rot_v, wq_v, wo_v, wg_v, wu_v, wd_v, q_v, s_v, p_v, f_v, own_v, hown_v,
           t1, r1, hh, t2, r2, yy, rx, ksem, vsem, wsem, send_sem, recv_sem, near_send, near_recv):
    me = lax.axis_index("tp")
    rows, d_model = x_v.shape
    chunks = rows // CHUNK
    cache = kbuf.shape[2]
    pairs = CHUNK // 2
    width = d_model // n
    *early, late, last = range(chunks)
    chips = n // 2
    chip, core = lax.div(me, 2), lax.rem(me, 2)

    def by_chip(phase, c):
        return isinstance(c, int) and (phase, c) in paired(early, late, last)

    barrier = pltpu.get_barrier_semaphore()
    for d in range(1, n):
        pl.semaphore_signal(barrier, inc=1, device_id={"tp": lax.rem(me + d, n)}, device_id_type=MESH)

    small = [(x_hbm, x_v), (wq_hbm, wq_v), (ga_hbm, ga_v), (rot_hbm, rot_v), (wo_hbm, wo_v), (gm_hbm, gm_v),
             (wg_hbm, wg_v), (wu_hbm, wu_v), (wd_hbm, wd_v)]

    def load(i):
        return pltpu.make_async_copy(small[i][0], small[i][1], wsem.at[i])

    def kv(hbm, buf, sem, c, j):
        slot = lax.rem(c, SLOTS)
        return pltpu.make_async_copy(hbm.at[pl.ds(c * CHUNK + 2 * j, 2)], buf.at[slot, pl.ds(2 * j, 2)], sem.at[slot, j])

    def item(c, i):
        c, i = c + i // (2 * pairs), i % (2 * pairs)
        return kv(k_hbm, kbuf, ksem, c, i) if i < pairs else kv(v_hbm, vbuf, vsem, c, i - pairs)

    def refill(c, i):
        ramp = 2 * i + pairs + 1 <= i + AHEAD

        @pl.when(c == 0)
        def _():
            for m in (2 * i + pairs, 2 * i + pairs + 1) if ramp else (i + AHEAD,):
                item(0, m).start()

        @pl.when((c > 0) & (c + (i + AHEAD) // (2 * pairs) < chunks))
        def _():
            item(c, i + AHEAD).start()

    for i in range(4):
        load(i).start()
    for i in range(FIRST):
        item(0, i).start()

    with jax.named_scope("wait_x"):
        for i in (0, 2):
            load(i).wait()
    for c in range(chunks):
        wide = x_v[c * CHUNK:(c + 1) * CHUNK, :].astype(F32)
        scale = lax.rsqrt(jnp.mean(wide * wide, -1, keepdims=True) + EPS)
        for k in range(n):
            block = pl.ds(k * width, width)
            a_v[c * CHUNK:(c + 1) * CHUNK, block] = (wide[:, k * width:(k + 1) * width] * scale * ga_v[k:k + 1, :].astype(F32)).astype(BF16)
    with jax.named_scope("wait_wq"):
        for i in (1, 3):
            load(i).wait()
    load(4).start()
    for i in range(FIRST, pairs):
        item(0, i).start()
    q = jnp.dot(a_v[...], wq_v[...], preferred_element_type=F32).astype(BF16).astype(F32)
    q_v[...] = (q * rot_v[0:1, :] + pltpu.roll(q, HEAD // 2, 1) * rot_v[1:2, :]).astype(BF16)

    row = lax.broadcasted_iota(jnp.int32, (CHUNK, HEAD), 0)

    def remote(source, target, send, recv, to):
        return pltpu.make_async_remote_copy(
            src_ref=source, dst_ref=target, send_sem=send, recv_sem=recv, device_id={"tp": to}, device_id_type=MESH)

    def send_all(phase, c, source, target):
        if by_chip(phase, c):
            for d in far_first(chips):
                there = lax.rem(chip + d, chips)
                remote(source(core, there), target(d), send_sem.at[phase, c], recv_sem.at[phase, c], 2 * there + core).start()
        else:
            for d in far_first(n):
                to = lax.rem(me + d, n)
                remote(source(lax.rem(to, 2), lax.div(to, 2)), target(d), send_sem.at[phase, c], recv_sem.at[phase, c], to).start()

    def tiles(phase, c):
        return r1.at[0, pl.ds(0, (chips if by_chip(phase, c) else n) - 1)]

    def arrived(phase, c):
        remote(tiles(phase, c), tiles(phase, c), send_sem.at[phase, c], recv_sem.at[phase, c], me).wait_recv()

    def near(phase, c, source, target):
        return remote(source, target, near_send.at[phase, c], near_recv.at[phase, c], me + 1 - 2 * core)

    def sent(phase, c):
        remote(tiles(phase, c), tiles(phase, c), send_sem.at[phase, c], recv_sem.at[phase, c], me).wait_send()
        if by_chip(phase, c):
            near(phase, c, rx.at[0], rx.at[0]).wait_send()

    def split(phase, c, term, t):
        for k in range(n):
            part = term[:, k * width:(k + 1) * width]
            f_v[c, k % 2, k // 2] = part
            t[c, k % 2, k // 2] = part.astype(BF16)
        if by_chip(phase, c):
            near(phase, c, t.at[c, 1 - core], rx.at[c]).start()

    def scatter(phase, c, t, r):
        if by_chip(phase, c):
            with jax.named_scope("wait_near"):
                near(phase, c, rx.at[c], rx.at[c]).wait_recv()
            for there in range(chips):
                part = f_v[c, core, there] + rx[c, there].astype(F32)
                f_v[c, core, there] = part
                t[c, core, there] = part.astype(BF16)
        own_v[phase // 2, c] = f_v[c, core, chip]
        send_all(phase, c, lambda i, there: t.at[c, i, there], lambda d: r.at[c, d - 1])

    def gathered(phase, c, r):
        with jax.named_scope("wait_terms"):
            arrived(phase, c)
        total = own_v[phase // 2, c]
        for d in range((chips if by_chip(phase, c) else n) - 1):
            total = total + r[c, d].astype(F32)
        return total

    def spread(phase, c, ref):
        send_all(phase, c, lambda i, there: ref.at[c, core, chip], lambda d: ref.at[c, core, chip])

    def relay(phase, c, ref):
        with jax.named_scope("wait_far"):
            arrived(phase, c)
        near(phase, c, ref.at[c, core], ref.at[c, core]).start()

    def complete(phase, c):
        if by_chip(phase, c):
            near(phase, c, rx.at[0], rx.at[0]).wait_recv()
        else:
            arrived(phase, c)

    def attention(c):
        slot = lax.rem(c, SLOTS)
        queries = q_v[pl.ds(pl.multiple_of(c * CHUNK, CHUNK), CHUNK), :].astype(F32)
        for j in range(pairs):
            with jax.named_scope("wait_k"):
                kv(k_hbm, kbuf, ksem, c, j).wait()
            refill(c, j)
            with jax.named_scope("scores"):
                both = jnp.concatenate([jnp.where(row == 2 * j, queries, 0.0), jnp.where(row == 2 * j + 1, queries, 0.0)], -1).astype(BF16)
                for t in range(0, cache, TILE):
                    keys = jnp.concatenate([kbuf[slot, 2 * j, t:t + TILE, :], kbuf[slot, 2 * j + 1, t:t + TILE, :]], -1)
                    part = lax.dot_general(both, keys, (((1,), (1,)), ((), ())), preferred_element_type=F32)
                    if j == 0:
                        s_v[:, t:t + TILE] = part
                    else:
                        s_v[:, t:t + TILE] += part

        @pl.when(c == 0)
        def _():
            load(4).wait()
            with jax.named_scope("barrier"):
                pl.semaphore_wait(barrier, n - 1)

        @pl.when(c >= 2)
        def _():
            finish_h(c - 2)

        with jax.named_scope("softmax"):
            scores = s_v[...] * HEAD**-0.5
            e = jnp.exp(scores - jnp.max(scores, -1, keepdims=True))
            p_v[...] = (e / jnp.sum(e, -1, keepdims=True)).astype(BF16)
        seen = jnp.zeros((CHUNK, HEAD), F32)
        for j in range(0, pairs, GROUP):
            with jax.named_scope("wait_v"):
                for i in range(j, j + GROUP):
                    kv(v_hbm, vbuf, vsem, c, i).wait()
            for i in range(j, j + GROUP):
                refill(c, pairs + i)
            if j + GROUP == pairs:
                @pl.when(c == chunks - 1)
                def _():
                    for i in range(5, 9):
                        load(i).start()

            with jax.named_scope("values"):
                values = jnp.concatenate([vbuf[slot, 2 * j + i] for i in range(2 * GROUP)], -1)
                each = jnp.dot(p_v[...], values, preferred_element_type=F32)
                for i in range(2 * GROUP):
                    seen = jnp.where(row == 2 * j + i, each[:, i * HEAD:(i + 1) * HEAD], seen)

        with jax.named_scope("wo"):
            split(0, c, jnp.dot(seen.astype(BF16), wo_v[...], preferred_element_type=F32), t1)
            scatter(0, c, t1, r1)

    def finish_h(c):
        mine = x_v[pl.ds(pl.multiple_of(c * CHUNK, CHUNK), CHUNK), pl.ds(pl.multiple_of(me * width, width), width)]
        h = (mine.astype(F32) + gathered(0, c, r1)).astype(BF16)
        hown_v[c] = h
        hh[c, core, chip] = h
        spread(1, c, hh)

    def normed(c):
        with jax.named_scope("wait_h"):
            complete(1, c)
        squares = jnp.zeros((CHUNK, width), F32)
        for k in range(n):
            wide = hh[c, k % 2, k // 2].astype(F32)
            squares = squares + wide * wide
        scale = lax.rsqrt(jnp.sum(squares, -1, keepdims=True) / d_model + EPS)
        return jnp.concatenate([(hh[c, k % 2, k // 2].astype(F32) * scale * gm_v[k:k + 1, :].astype(F32)).astype(BF16) for k in range(n)], -1)

    def mlp(*which):
        b = jnp.concatenate([normed(c) for c in which], 0)
        with jax.named_scope("mlp"):
            gate = jnp.dot(b, wg_v[...], preferred_element_type=F32)
            up = jnp.dot(b, wu_v[...], preferred_element_type=F32)
            hidden = (gate * jax.nn.sigmoid(gate) * up).astype(BF16)
            term = jnp.dot(hidden, wd_v[...], preferred_element_type=F32)
            for i, c in enumerate(which):
                split(2, c, term[i * CHUNK:(i + 1) * CHUNK], t2)

    def finish_y(c):
        yy[c, core, chip] = (hown_v[c].astype(F32) + gathered(2, c, r2)).astype(BF16)
        spread(3, c, yy)

    def step(c, carry):
        attention(c)
        return carry

    lax.fori_loop(0, chunks, step, 0)

    finish_h(late)
    with jax.named_scope("wait_w"):
        for i in range(5, 9):
            load(i).wait()
    mlp(*early)
    finish_h(last)
    if by_chip(1, late):
        relay(1, late, hh)
    mlp(late)
    for c in (*early, late):
        scatter(2, c, t2, r2)
    mlp(last)
    scatter(2, last, t2, r2)
    for c in range(chunks):
        finish_y(c)
    for c in range(chunks):
        if by_chip(3, c):
            relay(3, c, yy)
    for c in range(chunks):
        if c == last:
            for i in range(chunks):
                for phase in range(4 if i != last else 3):
                    sent(phase, i)
        with jax.named_scope("wait_y"):
            complete(3, c)
        for k in range(n):
            out_ref[c * CHUNK:(c + 1) * CHUNK, k * width:(k + 1) * width] = yy[c, k % 2, k // 2]
    sent(3, last)


def rotation(place):
    half = HEAD // 2
    angle = np.float64(place) * float(THETA) ** (-np.arange(half) / half)
    cos, sin = np.cos(angle), np.sin(angle)
    table = np.zeros((8, HEAD), np.float32)
    table[0], table[1] = np.concatenate([cos, cos]), np.concatenate([-sin, sin])
    return table


def solution(mesh):
    n = mesh.shape["tp"]

    def step(x, k_cache, v_cache, gain_a, wq, wo, gain_m, w_gate, w_up, w_down):
        rows, d_model = x.shape
        cache = k_cache.shape[1]
        chunks, hidden, width = rows // CHUNK, w_gate.shape[1], d_model // n
        anywhere = pl.BlockSpec(memory_space=pltpu.HBM)
        tiles = pltpu.VMEM((chunks, 2, n // 2, CHUNK, width), BF16)
        arrivals = pltpu.VMEM((chunks, n - 1, CHUNK, width), BF16)
        dma = pltpu.SemaphoreType.DMA
        return pl.pallas_call(
            functools.partial(kernel, n),
            out_shape=jax.ShapeDtypeStruct((rows, d_model), BF16),
            in_specs=[anywhere] * 11,
            out_specs=pl.BlockSpec(memory_space=pltpu.VMEM),
            scratch_shapes=[
                pltpu.VMEM((SLOTS, CHUNK, cache, HEAD), BF16),
                pltpu.VMEM((SLOTS, CHUNK, cache, HEAD), BF16),
                pltpu.VMEM((rows, d_model), BF16),
                pltpu.VMEM((rows, d_model), BF16),
                pltpu.VMEM((n, width), BF16),
                pltpu.VMEM((n, width), BF16),
                pltpu.VMEM((8, HEAD), F32),
                pltpu.VMEM(wq.shape, BF16),
                pltpu.VMEM(wo.shape, BF16),
                pltpu.VMEM((d_model, hidden), BF16),
                pltpu.VMEM((d_model, hidden), BF16),
                pltpu.VMEM((hidden, d_model), BF16),
                pltpu.VMEM((rows, HEAD), BF16),
                pltpu.VMEM((CHUNK, cache), F32),
                pltpu.VMEM((CHUNK, cache), BF16),
                pltpu.VMEM((chunks, 2, n // 2, CHUNK, width), F32),
                pltpu.VMEM((2, chunks, CHUNK, width), F32),
                pltpu.VMEM((chunks, CHUNK, width), BF16),
                tiles, arrivals, tiles, tiles, arrivals, tiles, pltpu.VMEM((chunks, n // 2, CHUNK, width), BF16),
                dma((SLOTS, CHUNK // 2)), dma((SLOTS, CHUNK // 2)), dma((9,)), *[dma((4, chunks))] * 4,
            ],
            compiler_params=pltpu.CompilerParams(collective_id=0, has_side_effects=True, vmem_limit_bytes=VMEM_LIMIT),
        )(*(pltpu.with_memory_space_constraint(a, pltpu.HBM) for a in (
            x, k_cache.reshape(rows, cache, HEAD), v_cache.reshape(rows, cache, HEAD), gain_a.reshape(n, width), wq, wo,
            gain_m.reshape(n, width), w_gate, w_up, w_down, jnp.asarray(rotation(cache - 1)))))

    states, cache, columns, rows_of = P("dp", None), P("dp", None, "tp", None), P(None, "tp"), P("tp", None)
    return jax.shard_map(
        step,
        mesh=mesh,
        in_specs=(states, cache, cache, P(None), columns, rows_of, P(None), columns, columns, rows_of),
        out_specs=states,
        check_vma=False,
    )
```

```python
import functools

import jax
import jax.numpy as jnp
import numpy as np
from jax import lax
from jax.experimental import pallas as pl
from jax.experimental.pallas import tpu as pltpu
from jax.sharding import PartitionSpec as P

HEAD = 128
THETA = 10000
CHUNK = 16
HALF = CHUNK // 2
SLOTS = 2
AHEAD = CHUNK
FIRST = 4
KEYS = 2
GROUP = 4
VMEM_LIMIT = 48 << 20
TILE = 256
EPS = 1e-6
MESH = pl.DeviceIdType.MESH
F32, BF16 = jnp.float32, jnp.bfloat16


def paired(early, mid, late):
    return [(1, mid), *((phase, c) for phase in (2, 3) for c in (*early, mid, late))]


def far_first(n):
    return sorted(range(1, n), key=lambda d: -min(d, n - d))


def kernel(n, x_hbm, k_hbm, v_hbm, ga_hbm, wq_hbm, wo_hbm, gm_hbm, wg_hbm, wu_hbm, wd_hbm, rot_hbm, out_ref,
           kbuf, vbuf, x_v, a_v, ga_v, gm_v, rot_v, wq_v, wo_v, wg_v, wu_v, wd_v, q_v, s_v, p_v, f_v, own_v, hown_v,
           t1, r1, hh, t2, r2, yy, rx, t1h, r1h, hhh, t2h, r2h, yyh, rxh, ksem, vsem, wsem, send_sem, recv_sem, near_recv):
    t1, r1, hh, t2, r2, yy, rx = (t1, t1h), (r1, r1h), (hh, hhh), (t2, t2h), (r2, r2h), (yy, yyh), (rx, rxh)
    me = lax.axis_index("tp")
    rows, d_model = x_v.shape
    blocks = rows // CHUNK
    chunks = blocks + 1
    cache = kbuf.shape[2]
    pairs = CHUNK // 2
    width = d_model // n
    *early, mid, late, last = range(chunks)
    chips = n // 2
    chip, core = lax.div(me, 2), lax.rem(me, 2)

    def whole(c):
        return not isinstance(c, int) or c < late

    def size(c):
        return CHUNK if whole(c) else HALF

    def at(refs, c):
        return refs[0].at[c] if whole(c) else refs[1].at[c - late]

    def by_chip(phase, c):
        return isinstance(c, int) and (phase, c) in paired(early, mid, late)

    barrier = pltpu.get_barrier_semaphore()
    for d in range(1, n):
        pl.semaphore_signal(barrier, inc=1, device_id={"tp": lax.rem(me + d, n)}, device_id_type=MESH)

    small = [(x_hbm, x_v), (wq_hbm, wq_v), (ga_hbm, ga_v), (rot_hbm, rot_v), (wo_hbm, wo_v), (gm_hbm, gm_v),
             (wg_hbm, wg_v), (wu_hbm, wu_v), (wd_hbm, wd_v)]

    def load(i):
        return pltpu.make_async_copy(small[i][0], small[i][1], wsem.at[i])

    def kv(hbm, buf, sem, c, j, count=1, group=1):
        slot = lax.rem(c, SLOTS)
        return pltpu.make_async_copy(
            hbm.at[pl.ds(c * CHUNK + 2 * j, 2 * count)], buf.at[slot, pl.ds(2 * j, 2 * count)], sem.at[slot, j // group])

    def item(c, i, halves=False):
        if halves:
            i = i // pairs * (pairs // 2) + i % (pairs // 2) + i % pairs // (pairs // 2) * pairs
        return kv(k_hbm, kbuf, ksem, c, i, 1, KEYS) if i < pairs else kv(v_hbm, vbuf, vsem, c, i - pairs, 1, GROUP)

    def refill(c, i):
        if isinstance(c, int):
            return

        @pl.when(c == 0)
        def _():
            for m in (2 * i + pairs, 2 * i + pairs + 1) if 2 * i + pairs + 1 <= i + AHEAD else (i + AHEAD,):
                item(m // AHEAD, m % AHEAD).start()

        @pl.when((c > 0) & (c < blocks - 2))
        def _():
            item(c + 1, i).start()

        @pl.when(c == blocks - 2)
        def _():
            item(c + 1, i, True).start()

    for i in range(4):
        load(i).start()
    for i in range(FIRST):
        item(0, i).start()

    with jax.named_scope("wait_x"):
        for i in (0, 2):
            load(i).wait()
    for c in range(blocks):
        wide = x_v[c * CHUNK:(c + 1) * CHUNK, :].astype(F32)
        scale = lax.rsqrt(jnp.mean(wide * wide, -1, keepdims=True) + EPS)
        for k in range(n):
            block = pl.ds(k * width, width)
            a_v[c * CHUNK:(c + 1) * CHUNK, block] = (wide[:, k * width:(k + 1) * width] * scale * ga_v[k:k + 1, :].astype(F32)).astype(BF16)
    with jax.named_scope("wait_wq"):
        for i in (1, 3):
            load(i).wait()
    load(4).start()
    for i in range(FIRST, pairs):
        item(0, i).start()
    q = jnp.dot(a_v[...], wq_v[...], preferred_element_type=F32).astype(BF16).astype(F32)
    q_v[...] = (q * rot_v[0:1, :] + pltpu.roll(q, HEAD // 2, 1) * rot_v[1:2, :]).astype(BF16).astype(F32)

    row = lax.broadcasted_iota(jnp.int32, (CHUNK, HEAD), 0)

    def remote(source, target, send, recv, to):
        return pltpu.make_async_remote_copy(
            src_ref=source, dst_ref=target, send_sem=send, recv_sem=recv, device_id={"tp": to}, device_id_type=MESH)

    def send_all(phase, c, source, target):
        if by_chip(phase, c):
            for d in far_first(chips):
                there = lax.rem(chip + d, chips)
                remote(source(core, there), target(d), send_sem, recv_sem.at[phase, c], 2 * there + core).start()
        else:
            for d in far_first(n):
                to = lax.rem(me + d, n)
                remote(source(lax.rem(to, 2), lax.div(to, 2)), target(d), send_sem, recv_sem.at[phase, c], to).start()

    def tiles(phase, c):
        return r1[0 if whole(c) else 1].at[0, pl.ds(0, (chips if by_chip(phase, c) else n) - 1)]

    def arrived(phase, c):
        remote(tiles(phase, c), tiles(phase, c), send_sem, recv_sem.at[phase, c], me).wait_recv()

    def near(phase, c, source, target):
        return remote(source, target, send_sem, near_recv.at[paired(early, mid, late).index((phase, c))], me + 1 - 2 * core)

    def all_sent():
        count = sum(size(c) * (chips - 1 + chips if by_chip(phase, c) else n - 1) for phase in range(4) for c in range(chunks))
        ref = kbuf.at[0, pl.ds(0, count // TILE), pl.ds(0, TILE)]
        remote(ref, ref, send_sem, recv_sem.at[0, 0], me).wait_send()

    def split(phase, c, term, t):
        for k in range(n):
            part = term[:, k * width:(k + 1) * width]
            f_v[c, k % 2, k // 2, :size(c)] = part
            at(t, c)[k % 2, k // 2] = part.astype(BF16)
        if by_chip(phase, c):
            near(phase, c, at(t, c).at[1 - core], at(rx, c)).start()

    def scatter(phase, c, t, r):
        if by_chip(phase, c):
            with jax.named_scope("wait_near"):
                near(phase, c, at(rx, c), at(rx, c)).wait_recv()
            for there in range(chips):
                part = f_v[c, core, there, :size(c)] + at(rx, c)[there].astype(F32)
                f_v[c, core, there, :size(c)] = part
                at(t, c)[core, there] = part.astype(BF16)
        own_v[phase // 2, c, :size(c)] = f_v[c, core, chip, :size(c)]
        send_all(phase, c, lambda i, there: at(t, c).at[i, there], lambda d: at(r, c).at[d - 1])

    def gathered(phase, c, r):
        with jax.named_scope("wait_terms"):
            arrived(phase, c)
        total = own_v[phase // 2, c, :size(c)]
        for d in range((chips if by_chip(phase, c) else n) - 1):
            total = total + at(r, c)[d].astype(F32)
        return total

    def spread(phase, c, ref):
        send_all(phase, c, lambda i, there: at(ref, c).at[core, chip], lambda d: at(ref, c).at[core, chip])

    def relay(phase, c, ref):
        with jax.named_scope("wait_far"):
            arrived(phase, c)
        near(phase, c, at(ref, c).at[core], at(ref, c).at[core]).start()

    def complete(phase, c):
        if by_chip(phase, c):
            near(phase, c, at(rx, c), at(rx, c)).wait_recv()
        else:
            arrived(phase, c)

    def attention(c, half=None):
        slot = lax.rem(c, SLOTS)
        queries = q_v[pl.ds(pl.multiple_of(c * CHUNK, CHUNK), CHUNK), :]
        start, stop = (0, pairs) if half is None else (half * pairs // 2, (half + 1) * pairs // 2)
        for j in range(start, stop):
            if j % KEYS == 0:
                with jax.named_scope("wait_k"):
                    kv(k_hbm, kbuf, ksem, c, j, KEYS, KEYS).wait()
                for i in range(j, j + KEYS):
                    refill(c, i)
            with jax.named_scope("scores"):
                both = jnp.concatenate([jnp.where(row == 2 * j, queries, 0.0), jnp.where(row == 2 * j + 1, queries, 0.0)], -1).astype(BF16)
                for t in range(0, cache, TILE):
                    keys = jnp.concatenate([kbuf[slot, 2 * j, t:t + TILE, :], kbuf[slot, 2 * j + 1, t:t + TILE, :]], -1)
                    part = lax.dot_general(both, keys, (((1,), (1,)), ((), ())), preferred_element_type=F32)
                    if j == start:
                        s_v[:, t:t + TILE] = part
                    else:
                        s_v[:, t:t + TILE] += part

        if half is None:
            @pl.when(c == 0)
            def _():
                load(4).wait()
                with jax.named_scope("barrier"):
                    pl.semaphore_wait(barrier, n - 1)

            @pl.when(c >= 2)
            def _():
                finish_h(c - 2)
        elif half == 0:
            finish_h(c - 2)

        with jax.named_scope("softmax"):
            scores = s_v[...] * HEAD**-0.5
            e = jnp.exp(scores - jnp.max(scores, -1, keepdims=True))
            p_v[...] = (e / jnp.sum(e, -1, keepdims=True)).astype(BF16)
        seen = jnp.zeros((CHUNK, HEAD), F32)
        for j in range(start, stop, GROUP):
            with jax.named_scope("wait_v"):
                kv(v_hbm, vbuf, vsem, c, j, GROUP, GROUP).wait()
            for i in range(j, j + GROUP):
                refill(c, pairs + i)
            if half == 1:
                for i in range(5, 9):
                    load(i).start()

            with jax.named_scope("values"):
                values = jnp.concatenate([vbuf[slot, 2 * j + i] for i in range(2 * GROUP)], -1)
                each = jnp.dot(p_v[...], values, preferred_element_type=F32)
                for i in range(2 * GROUP):
                    seen = jnp.where(row == 2 * j + i, each[:, i * HEAD:(i + 1) * HEAD], seen)

        with jax.named_scope("wo"):
            term = jnp.dot(seen.astype(BF16), wo_v[...], preferred_element_type=F32)
            if half is not None:
                c, term = c + half, term[half * HALF:(half + 1) * HALF]
            split(0, c, term, t1)
            scatter(0, c, t1, r1)

    def finish_h(c):
        block = c if whole(c) else blocks - 1
        mine = x_v[pl.ds(pl.multiple_of(block * CHUNK, CHUNK), CHUNK), pl.ds(pl.multiple_of(me * width, width), width)].astype(F32)
        if not whole(c):
            mine = mine[(c - late) * HALF:(c - late + 1) * HALF]
        h = (mine + gathered(0, c, r1)).astype(BF16)
        hown_v[c, :size(c)] = h.astype(F32)
        at(hh, c)[core, chip] = h
        spread(1, c, hh)

    def normed(c):
        with jax.named_scope("wait_h"):
            complete(1, c)
        tiles = [at(hh, c)[k % 2, k // 2].astype(F32) for k in range(n)]
        scale = lax.rsqrt(jnp.sum(sum(wide * wide for wide in tiles), -1, keepdims=True) / d_model + EPS)
        return jnp.concatenate([wide * scale * gm_v[k:k + 1, :].astype(F32) for k, wide in enumerate(tiles)], -1)

    def mlp(*which):
        b = [normed(c) for c in which]
        if sum(size(c) for c in which) % CHUNK:
            b.append(jnp.zeros((HALF, d_model), F32))
        b = jnp.concatenate(b, 0).astype(BF16)
        with jax.named_scope("mlp"):
            gate = jnp.dot(b, wg_v[...], preferred_element_type=F32)
            up = jnp.dot(b, wu_v[...], preferred_element_type=F32)
            hidden = (gate * jax.nn.sigmoid(gate) * up).astype(BF16)
            term = jnp.dot(hidden, wd_v[...], preferred_element_type=F32)
            row = 0
            for c in which:
                split(2, c, term[row:row + size(c)], t2)
                row += size(c)

    def finish_y(c):
        at(yy, c)[core, chip] = (hown_v[c, :size(c)] + gathered(2, c, r2)).astype(BF16)
        spread(3, c, yy)

    def step(c, carry):
        attention(c)
        return carry

    lax.fori_loop(0, blocks - 1, step, 0)
    attention(blocks - 1, 0)
    attention(blocks - 1, 1)

    finish_h(mid)
    finish_h(late)
    with jax.named_scope("wait_w"):
        for i in range(5, 9):
            load(i).wait()
    mlp(*early)
    finish_h(last)
    for c in early:
        scatter(2, c, t2, r2)
    relay(1, mid, hh)
    mlp(mid, late)
    for c in (mid, late):
        scatter(2, c, t2, r2)
    mlp(last)
    scatter(2, last, t2, r2)
    for c in range(chunks):
        finish_y(c)
    for c in range(last):
        relay(3, c, yy)

    for c in (*early, mid):
        with jax.named_scope("wait_y"):
            complete(3, c)
        for k in range(n):
            out_ref[c * CHUNK:(c + 1) * CHUNK, k * width:(k + 1) * width] = at(yy, c)[k % 2, k // 2]
    with jax.named_scope("wait_y"):
        complete(3, late)
        complete(3, last)
    for k in range(n):
        both = [at(yy, c)[k % 2, k // 2].astype(F32) for c in (late, last)]
        out_ref[(blocks - 1) * CHUNK:, k * width:(k + 1) * width] = jnp.concatenate(both, 0).astype(BF16)
    with jax.named_scope("sent"):
        all_sent()


def rotation(place):
    half = HEAD // 2
    angle = np.float64(place) * float(THETA) ** (-np.arange(half) / half)
    cos, sin = np.cos(angle), np.sin(angle)
    table = np.zeros((8, HEAD), np.float32)
    table[0], table[1] = np.concatenate([cos, cos]), np.concatenate([-sin, sin])
    return table


def solution(mesh):
    n = mesh.shape["tp"]

    def step(x, k_cache, v_cache, gain_a, wq, wo, gain_m, w_gate, w_up, w_down):
        rows, d_model = x.shape
        cache = k_cache.shape[1]
        chunks, hidden, width = rows // CHUNK + 1, w_gate.shape[1], d_model // n
        anywhere = pl.BlockSpec(memory_space=pltpu.HBM)
        exchanged = []
        for parts, m in ((chunks - 2, CHUNK), (2, HALF)):
            tiles, arrivals = pltpu.VMEM((parts, 2, n // 2, m, width), BF16), pltpu.VMEM((parts, n - 1, m, width), BF16)
            exchanged += [tiles, arrivals, tiles, tiles, arrivals, tiles, pltpu.VMEM((parts, n // 2, m, width), BF16)]
        dma = pltpu.SemaphoreType.DMA
        return pl.pallas_call(
            functools.partial(kernel, n),
            out_shape=jax.ShapeDtypeStruct((rows, d_model), BF16),
            in_specs=[anywhere] * 11,
            out_specs=pl.BlockSpec(memory_space=pltpu.VMEM),
            scratch_shapes=[
                pltpu.VMEM((SLOTS, CHUNK, cache, HEAD), BF16),
                pltpu.VMEM((SLOTS, CHUNK, cache, HEAD), BF16),
                pltpu.VMEM((rows, d_model), BF16),
                pltpu.VMEM((rows, d_model), BF16),
                pltpu.VMEM((n, width), BF16),
                pltpu.VMEM((n, width), BF16),
                pltpu.VMEM((8, HEAD), F32),
                pltpu.VMEM(wq.shape, BF16),
                pltpu.VMEM(wo.shape, BF16),
                pltpu.VMEM((d_model, hidden), BF16),
                pltpu.VMEM((d_model, hidden), BF16),
                pltpu.VMEM((hidden, d_model), BF16),
                pltpu.VMEM((rows, HEAD), F32),
                pltpu.VMEM((CHUNK, cache), F32),
                pltpu.VMEM((CHUNK, cache), BF16),
                pltpu.VMEM((chunks, 2, n // 2, CHUNK, width), F32),
                pltpu.VMEM((2, chunks, CHUNK, width), F32),
                pltpu.VMEM((chunks, CHUNK, width), F32),
                *exchanged,
                dma((SLOTS, HALF // KEYS)), dma((SLOTS, HALF // GROUP)), dma((9,)), dma(()), dma((4, chunks)), dma((2 * chunks - 1,)),
            ],
            compiler_params=pltpu.CompilerParams(collective_id=0, has_side_effects=True, vmem_limit_bytes=VMEM_LIMIT),
        )(*(pltpu.with_memory_space_constraint(a, pltpu.HBM) for a in (
            x, k_cache.reshape(rows, cache, HEAD), v_cache.reshape(rows, cache, HEAD), gain_a.reshape(n, width), wq, wo,
            gain_m.reshape(n, width), w_gate, w_up, w_down, jnp.asarray(rotation(cache - 1)))))

    states, cache, columns, rows_of = P("dp", None), P("dp", None, "tp", None), P(None, "tp"), P("tp", None)
    return jax.shard_map(
        step,
        mesh=mesh,
        in_specs=(states, cache, cache, P(None), columns, rows_of, P(None), columns, columns, rows_of),
        out_specs=states,
        check_vma=False,
    )
```

```python
import functools

import jax
import jax.numpy as jnp
import numpy as np
from jax import lax
from jax.experimental import pallas as pl
from jax.experimental.pallas import tpu as pltpu
from jax.sharding import PartitionSpec as P

HEAD = 128
THETA = 10000
CHUNK = 16
HALF = CHUNK // 2
SLOTS = 2
AHEAD = CHUNK
FIRST = 4
KEYS = 2
GROUP = 4
VMEM_LIMIT = 48 << 20
TILE = 256
EPS = 1e-6
MESH = pl.DeviceIdType.MESH
F32, BF16 = jnp.float32, jnp.bfloat16


def paired(early, mid, late):
    return [(1, mid), *((phase, c) for phase in (2, 3) for c in (*early, mid, late))]


def far_first(n):
    return sorted(range(1, n), key=lambda d: -min(d, n - d))


def kernel(n, x_hbm, k_hbm, v_hbm, ga_hbm, wq_hbm, wo_hbm, gm_hbm, wg_hbm, wu_hbm, wd_hbm, rot_hbm, out_ref,
           kbuf, vbuf, x_v, a_v, ga_v, gm_v, rot_v, wq_v, wo_v, wg_v, wu_v, wd_v, q_v, s_v, p_v, f_v, own_v, hown_v,
           t1, r1, hh, t2, r2, yy, rx, t1h, r1h, hhh, t2h, r2h, yyh, rxh, ksem, vsem, wsem, send_sem, recv_sem, near_recv):
    t1, r1, hh, t2, r2, yy, rx = (t1, t1h), (r1, r1h), (hh, hhh), (t2, t2h), (r2, r2h), (yy, yyh), (rx, rxh)
    me = lax.axis_index("tp")
    rows, d_model = x_v.shape
    blocks = rows // CHUNK
    chunks = blocks + 1
    cache = kbuf.shape[2]
    pairs = CHUNK // 2
    width = d_model // n
    *early, mid, late, last = range(chunks)
    chips = n // 2
    chip, core = lax.div(me, 2), lax.rem(me, 2)

    def whole(c):
        return not isinstance(c, int) or c < late

    def size(c):
        return CHUNK if whole(c) else HALF

    def at(refs, c):
        return refs[0].at[c] if whole(c) else refs[1].at[c - late]

    def by_chip(phase, c):
        return isinstance(c, int) and (phase, c) in paired(early, mid, late)

    barrier = pltpu.get_barrier_semaphore()
    for d in range(1, n):
        pl.semaphore_signal(barrier, inc=1, device_id={"tp": lax.rem(me + d, n)}, device_id_type=MESH)

    small = [(x_hbm, x_v), (wq_hbm, wq_v), (ga_hbm, ga_v), (rot_hbm, rot_v), (wo_hbm, wo_v), (gm_hbm, gm_v),
             (wg_hbm, wg_v), (wu_hbm, wu_v), (wd_hbm, wd_v)]

    def load(i):
        return pltpu.make_async_copy(small[i][0], small[i][1], wsem.at[i])

    def kv(hbm, buf, sem, c, j, count=1, group=1):
        slot = lax.rem(c, SLOTS)
        return pltpu.make_async_copy(
            hbm.at[pl.ds(c * CHUNK + 2 * j, 2 * count)], buf.at[slot, pl.ds(2 * j, 2 * count)], sem.at[slot, j // group])

    def item(c, i, halves=False):
        if halves:
            i = i // pairs * (pairs // 2) + i % (pairs // 2) + i % pairs // (pairs // 2) * pairs
        return kv(k_hbm, kbuf, ksem, c, i, 1, KEYS) if i < pairs else kv(v_hbm, vbuf, vsem, c, i - pairs, 1, GROUP)

    def refill(c, i):
        if isinstance(c, int):
            return

        @pl.when(c == 0)
        def _():
            for m in (2 * i + pairs, 2 * i + pairs + 1) if 2 * i + pairs + 1 <= i + AHEAD else (i + AHEAD,):
                item(m // AHEAD, m % AHEAD).start()

        @pl.when((c > 0) & (c < blocks - 2))
        def _():
            item(c + 1, i).start()

        @pl.when(c == blocks - 2)
        def _():
            item(c + 1, i, True).start()

    for i in range(4):
        load(i).start()
    for i in range(FIRST):
        item(0, i).start()

    with jax.named_scope("wait_x"):
        for i in (0, 2):
            load(i).wait()
    for c in range(blocks):
        wide = x_v[c * CHUNK:(c + 1) * CHUNK, :].astype(F32)
        scale = lax.rsqrt(jnp.mean(wide * wide, -1, keepdims=True) + EPS)
        for k in range(n):
            block = pl.ds(k * width, width)
            a_v[c * CHUNK:(c + 1) * CHUNK, block] = (wide[:, k * width:(k + 1) * width] * scale * ga_v[k:k + 1, :].astype(F32)).astype(BF16)
    with jax.named_scope("wait_wq"):
        for i in (1, 3):
            load(i).wait()
    load(4).start()
    for i in range(FIRST, pairs):
        item(0, i).start()
    q = jnp.dot(a_v[...], wq_v[...], preferred_element_type=F32).astype(BF16).astype(F32)
    q_v[...] = (q * rot_v[0:1, :] + pltpu.roll(q, HEAD // 2, 1) * rot_v[1:2, :]).astype(BF16).astype(F32)

    row = lax.broadcasted_iota(jnp.int32, (CHUNK, HEAD), 0)

    def remote(source, target, send, recv, to):
        return pltpu.make_async_remote_copy(
            src_ref=source, dst_ref=target, send_sem=send, recv_sem=recv, device_id={"tp": to}, device_id_type=MESH)

    def send_all(phase, c, source, target):
        if by_chip(phase, c):
            for d in far_first(chips):
                there = lax.rem(chip + d, chips)
                remote(source(core, there), target(d), send_sem, recv_sem.at[phase, c], 2 * there + core).start()
        else:
            for d in far_first(n):
                to = lax.rem(me + d, n)
                remote(source(lax.rem(to, 2), lax.div(to, 2)), target(d), send_sem, recv_sem.at[phase, c], to).start()

    def tiles(phase, c):
        return r1[0 if whole(c) else 1].at[0, pl.ds(0, (chips if by_chip(phase, c) else n) - 1)]

    def arrived(phase, c):
        remote(tiles(phase, c), tiles(phase, c), send_sem, recv_sem.at[phase, c], me).wait_recv()

    def near(phase, c, source, target):
        return remote(source, target, send_sem, near_recv.at[paired(early, mid, late).index((phase, c))], me + 1 - 2 * core)

    def all_sent():
        count = sum(size(c) * (chips - 1 + chips if by_chip(phase, c) else n - 1) for phase in range(4) for c in range(chunks))
        ref = kbuf.at[0, pl.ds(0, count // TILE), pl.ds(0, TILE)]
        remote(ref, ref, send_sem, recv_sem.at[0, 0], me).wait_send()

    def split(phase, c, term, t):
        for k in range(n):
            part = term[:, k * width:(k + 1) * width]
            f_v[c, k % 2, k // 2, :size(c)] = part
            at(t, c)[k % 2, k // 2] = part.astype(BF16)
        if by_chip(phase, c):
            near(phase, c, at(t, c).at[1 - core], at(rx, c)).start()

    def scatter(phase, c, t, r):
        if by_chip(phase, c):
            with jax.named_scope("wait_near"):
                near(phase, c, at(rx, c), at(rx, c)).wait_recv()
            for there in range(chips):
                part = f_v[c, core, there, :size(c)] + at(rx, c)[there].astype(F32)
                f_v[c, core, there, :size(c)] = part
                at(t, c)[core, there] = part.astype(BF16)
        own_v[phase // 2, c, :size(c)] = f_v[c, core, chip, :size(c)]
        send_all(phase, c, lambda i, there: at(t, c).at[i, there], lambda d: at(r, c).at[d - 1])

    def gathered(phase, c, r):
        with jax.named_scope("wait_terms"):
            arrived(phase, c)
        total = own_v[phase // 2, c, :size(c)]
        for d in range((chips if by_chip(phase, c) else n) - 1):
            total = total + at(r, c)[d].astype(F32)
        return total

    def spread(phase, c, ref):
        send_all(phase, c, lambda i, there: at(ref, c).at[core, chip], lambda d: at(ref, c).at[core, chip])

    def relay(phase, c, ref):
        with jax.named_scope("wait_far"):
            arrived(phase, c)
        near(phase, c, at(ref, c).at[core], at(ref, c).at[core]).start()

    def complete(phase, c):
        if by_chip(phase, c):
            near(phase, c, at(rx, c), at(rx, c)).wait_recv()
        else:
            arrived(phase, c)

    def attention(c, half=None):
        slot = lax.rem(c, SLOTS)
        queries = q_v[pl.ds(pl.multiple_of(c * CHUNK, CHUNK), CHUNK), :]
        start, stop = (0, pairs) if half is None else (half * pairs // 2, (half + 1) * pairs // 2)
        for j in range(start, stop):
            if j % KEYS == 0:
                with jax.named_scope("wait_k"):
                    kv(k_hbm, kbuf, ksem, c, j, KEYS, KEYS).wait()
                for i in range(j, j + KEYS):
                    refill(c, i)
                if half == 1 and j == start:
                    for i in range(5, 9):
                        load(i).start()
            with jax.named_scope("scores"):
                both = jnp.concatenate([jnp.where(row == 2 * j, queries, 0.0), jnp.where(row == 2 * j + 1, queries, 0.0)], -1).astype(BF16)
                for t in range(0, cache, TILE):
                    keys = jnp.concatenate([kbuf[slot, 2 * j, t:t + TILE, :], kbuf[slot, 2 * j + 1, t:t + TILE, :]], -1)
                    part = lax.dot_general(both, keys, (((1,), (1,)), ((), ())), preferred_element_type=F32)
                    if j == start:
                        s_v[:, t:t + TILE] = part
                    else:
                        s_v[:, t:t + TILE] += part

        if half is None:
            @pl.when(c == 0)
            def _():
                load(4).wait()
                with jax.named_scope("barrier"):
                    pl.semaphore_wait(barrier, n - 1)

            @pl.when(c >= 2)
            def _():
                finish_h(c - 2)
        elif half == 0:
            finish_h(c - 2)

        with jax.named_scope("softmax"):
            scores = s_v[...] * HEAD**-0.5
            e = jnp.exp(scores - jnp.max(scores, -1, keepdims=True))
            p_v[...] = (e / jnp.sum(e, -1, keepdims=True)).astype(BF16)
        seen = jnp.zeros((CHUNK, HEAD), F32)
        for j in range(start, stop, GROUP):
            with jax.named_scope("wait_v"):
                kv(v_hbm, vbuf, vsem, c, j, GROUP, GROUP).wait()
            for i in range(j, j + GROUP):
                refill(c, pairs + i)

            with jax.named_scope("values"):
                values = jnp.concatenate([vbuf[slot, 2 * j + i] for i in range(2 * GROUP)], -1)
                each = jnp.dot(p_v[...], values, preferred_element_type=F32)
                for i in range(2 * GROUP):
                    seen = jnp.where(row == 2 * j + i, each[:, i * HEAD:(i + 1) * HEAD], seen)

        with jax.named_scope("wo"):
            term = jnp.dot(seen.astype(BF16), wo_v[...], preferred_element_type=F32)
            if half is not None:
                c, term = c + half, term[half * HALF:(half + 1) * HALF]
            split(0, c, term, t1)
            scatter(0, c, t1, r1)

    def finish_h(c):
        block = c if whole(c) else blocks - 1
        mine = x_v[pl.ds(pl.multiple_of(block * CHUNK, CHUNK), CHUNK), pl.ds(pl.multiple_of(me * width, width), width)].astype(F32)
        if not whole(c):
            mine = mine[(c - late) * HALF:(c - late + 1) * HALF]
        h = (mine + gathered(0, c, r1)).astype(BF16)
        hown_v[c, :size(c)] = h.astype(F32)
        at(hh, c)[core, chip] = h
        spread(1, c, hh)

    def normed(c):
        with jax.named_scope("wait_h"):
            complete(1, c)
        tiles = [at(hh, c)[k % 2, k // 2].astype(F32) for k in range(n)]
        scale = lax.rsqrt(jnp.sum(sum(wide * wide for wide in tiles), -1, keepdims=True) / d_model + EPS)
        return jnp.concatenate([wide * scale * gm_v[k:k + 1, :].astype(F32) for k, wide in enumerate(tiles)], -1)

    def mlp(*which):
        b = [normed(c) for c in which]
        if sum(size(c) for c in which) % CHUNK:
            b.append(jnp.zeros((HALF, d_model), F32))
        b = jnp.concatenate(b, 0).astype(BF16)
        with jax.named_scope("mlp"):
            gate = jnp.dot(b, wg_v[...], preferred_element_type=F32)
            up = jnp.dot(b, wu_v[...], preferred_element_type=F32)
            hidden = (gate * jax.nn.sigmoid(gate) * up).astype(BF16)
            term = jnp.dot(hidden, wd_v[...], preferred_element_type=F32)
            row = 0
            for c in which:
                split(2, c, term[row:row + size(c)], t2)
                row += size(c)

    def finish_y(c):
        at(yy, c)[core, chip] = (hown_v[c, :size(c)] + gathered(2, c, r2)).astype(BF16)
        spread(3, c, yy)

    def step(c, carry):
        attention(c)
        return carry

    lax.fori_loop(0, blocks - 1, step, 0)
    attention(blocks - 1, 0)
    attention(blocks - 1, 1)

    finish_h(mid)
    finish_h(late)
    with jax.named_scope("wait_w"):
        for i in range(5, 9):
            load(i).wait()
    mlp(*early)
    finish_h(last)
    for c in early:
        scatter(2, c, t2, r2)
    relay(1, mid, hh)
    mlp(mid, late)
    for c in (mid, late):
        scatter(2, c, t2, r2)
    mlp(last)
    scatter(2, last, t2, r2)
    for c in range(chunks):
        finish_y(c)
    for c in range(last):
        relay(3, c, yy)

    for c in (*early, mid):
        with jax.named_scope("wait_y"):
            complete(3, c)
        for k in range(n):
            out_ref[c * CHUNK:(c + 1) * CHUNK, k * width:(k + 1) * width] = at(yy, c)[k % 2, k // 2]
    with jax.named_scope("wait_y"):
        complete(3, late)
        complete(3, last)
    for k in range(n):
        both = [at(yy, c)[k % 2, k // 2].astype(F32) for c in (late, last)]
        out_ref[(blocks - 1) * CHUNK:, k * width:(k + 1) * width] = jnp.concatenate(both, 0).astype(BF16)
    with jax.named_scope("sent"):
        all_sent()


def rotation(place):
    half = HEAD // 2
    angle = np.float64(place) * float(THETA) ** (-np.arange(half) / half)
    cos, sin = np.cos(angle), np.sin(angle)
    table = np.zeros((8, HEAD), np.float32)
    table[0], table[1] = np.concatenate([cos, cos]), np.concatenate([-sin, sin])
    return table


def solution(mesh):
    n = mesh.shape["tp"]

    def step(x, k_cache, v_cache, gain_a, wq, wo, gain_m, w_gate, w_up, w_down):
        rows, d_model = x.shape
        cache = k_cache.shape[1]
        chunks, hidden, width = rows // CHUNK + 1, w_gate.shape[1], d_model // n
        anywhere = pl.BlockSpec(memory_space=pltpu.HBM)
        exchanged = []
        for parts, m in ((chunks - 2, CHUNK), (2, HALF)):
            tiles, arrivals = pltpu.VMEM((parts, 2, n // 2, m, width), BF16), pltpu.VMEM((parts, n - 1, m, width), BF16)
            exchanged += [tiles, arrivals, tiles, tiles, arrivals, tiles, pltpu.VMEM((parts, n // 2, m, width), BF16)]
        dma = pltpu.SemaphoreType.DMA
        return pl.pallas_call(
            functools.partial(kernel, n),
            out_shape=jax.ShapeDtypeStruct((rows, d_model), BF16),
            in_specs=[anywhere] * 11,
            out_specs=pl.BlockSpec(memory_space=pltpu.VMEM),
            scratch_shapes=[
                pltpu.VMEM((SLOTS, CHUNK, cache, HEAD), BF16),
                pltpu.VMEM((SLOTS, CHUNK, cache, HEAD), BF16),
                pltpu.VMEM((rows, d_model), BF16),
                pltpu.VMEM((rows, d_model), BF16),
                pltpu.VMEM((n, width), BF16),
                pltpu.VMEM((n, width), BF16),
                pltpu.VMEM((8, HEAD), F32),
                pltpu.VMEM(wq.shape, BF16),
                pltpu.VMEM(wo.shape, BF16),
                pltpu.VMEM((d_model, hidden), BF16),
                pltpu.VMEM((d_model, hidden), BF16),
                pltpu.VMEM((hidden, d_model), BF16),
                pltpu.VMEM((rows, HEAD), F32),
                pltpu.VMEM((CHUNK, cache), F32),
                pltpu.VMEM((CHUNK, cache), BF16),
                pltpu.VMEM((chunks, 2, n // 2, CHUNK, width), F32),
                pltpu.VMEM((2, chunks, CHUNK, width), F32),
                pltpu.VMEM((chunks, CHUNK, width), F32),
                *exchanged,
                dma((SLOTS, HALF // KEYS)), dma((SLOTS, HALF // GROUP)), dma((9,)), dma(()), dma((4, chunks)), dma((2 * chunks - 1,)),
            ],
            compiler_params=pltpu.CompilerParams(collective_id=0, has_side_effects=True, vmem_limit_bytes=VMEM_LIMIT),
        )(*(pltpu.with_memory_space_constraint(a, pltpu.HBM) for a in (
            x, k_cache.reshape(rows, cache, HEAD), v_cache.reshape(rows, cache, HEAD), gain_a.reshape(n, width), wq, wo,
            gain_m.reshape(n, width), w_gate, w_up, w_down, jnp.asarray(rotation(cache - 1)))))

    states, cache, columns, rows_of = P("dp", None), P("dp", None, "tp", None), P(None, "tp"), P("tp", None)
    return jax.shard_map(
        step,
        mesh=mesh,
        in_specs=(states, cache, cache, P(None), columns, rows_of, P(None), columns, columns, rows_of),
        out_specs=states,
        check_vma=False,
    )
```
